32 devices in a mesh: dp: 2 (over x), section: 4 (over z), tensor: 4 (over y, core).
Axes of the slice: x: 2, y: 2, z: 4, core: 2. Of those that a mesh axis runs over, the one named last changes fastest.
Arguments:
- cotangent: bfloat16 [2, 64, 6144], P(None, 'tensor', 'dp'), may hold values from -6 to 6
- inputs: bfloat16 [4, 2, 64, 6144], P('section', None, 'tensor', 'dp'), may hold values from -6 to 6
- queries: bfloat16 [4, 2, 64, 6144], P('section', None, None, 'tensor'), may hold values from -256 to 256
- keys: bfloat16 [4, 2, 64, 6144], P('section', None, None, 'tensor'), may hold values from -8 to 8
- context: bfloat16 [4, 2, 64, 6144], P('section', None, None, 'tensor'), may hold values from -6 to 6
- value_weight: bfloat16 [4, 6144, 6144], P('section', 'dp', 'tensor'), may hold values from -0.078125 to 0.078125
- out_weight: bfloat16 [4, 6144, 6144], P('section', 'tensor', 'dp'), may hold values from -0.078125 to 0.078125
Outputs:
- section_grads: bfloat16 [4, 2, 64, 6144], P('section', None, 'tensor', 'dp')
- value_weight_grad: bfloat16 [4, 6144, 6144], P('section', 'dp', 'tensor')
- out_weight_grad: bfloat16 [4, 6144, 6144], P('section', 'tensor', 'dp')
The draws below stay inside these ranges and needn't reach their ends.
All inputs are finite; a program needn't handle non-finite values.
Results may differ from the reference program's by a relative error of at most 0.018.
Values may be sent and summed in bfloat16 or wider, within the bound.
No kernel may reach another device: no remote copies, remote signals or barrier semaphores. Data moves between devices by JAX's collectives and lax.ppermute only.
A program may use at most 128 MiB of HBM per device.

```python
import jax
import jax.numpy as jnp
from jax import lax

D = 6144
HEAD_DIM = 128
SEQ = 64
MICRO = 2
LAYERS = 4


def paired_draw(key):
    base = jax.random.fold_in(key, 7)
    key_query, key_key = jax.random.split(base, 2)
    shape = (LAYERS, MICRO, SEQ, D)
    query_all = jnp.clip(jax.random.normal(key_query, shape, jnp.float32), -5.0, 5.0)
    key_all = jnp.clip(jax.random.normal(key_key, shape, jnp.float32), -5.0, 5.0)
    return (query_all, key_all)


def draw_queries(key, part):
    return paired_draw(key)[0].astype(jnp.bfloat16)


def draw_keys(key, part):
    return paired_draw(key)[1].astype(jnp.bfloat16)


def level_of(key, dims, shards, least, largest):
    loudness = 1.0
    for position, parts in shards:
        steps = jax.random.uniform(jax.random.fold_in(jax.random.fold_in(key, 6), position), (parts,), jnp.float32, least / len(shards), largest / len(shards))
        loudness = loudness * jnp.repeat(jnp.exp(steps), dims[position] // parts).reshape((-1,) + (1,) * (len(dims) - 1 - position))
    return loudness


def gaussian(rng, dims, scale, bound, shards=(), dtype=jnp.bfloat16):
    values = jax.random.normal(rng, dims, jnp.float32) * scale
    if len(shards) > 0:
        values = level_of(rng, dims, shards, -0.22, 0.18) * values
    return jnp.clip(values, min=-bound, max=bound).astype(dtype)


def setup_inputs(seed: int = 0) -> dict:
    key_of = jax.random.split(jax.random.key(seed), 8)
    cotangent = gaussian(key_of[0], (MICRO, SEQ, D), 1.0, 6.0, ((1, 4), (2, 2)))
    inputs = gaussian(key_of[1], (LAYERS, MICRO, SEQ, D), 1.0, 6.0, ((0, 4), (2, 4), (3, 2)))
    queries = draw_queries(jax.random.fold_in(key_of[7], 71), 0)
    keys = draw_keys(jax.random.fold_in(key_of[7], 71), 0)
    context = gaussian(key_of[4], (LAYERS, MICRO, SEQ, D), 1.0, 6.0, ((0, 4), (3, 4)))
    value_weight = gaussian(key_of[5], (LAYERS, D, D), D ** -0.5, 0.078125, ((0, 4), (1, 2), (2, 4)))
    out_weight = gaussian(key_of[6], (LAYERS, D, D), D ** -0.5, 0.078125, ((0, 4), (1, 4), (2, 2)))
    return {"cotangent": cotangent, "inputs": inputs, "queries": queries, "keys": keys, "context": context, "value_weight": value_weight, "out_weight": out_weight}


def attention_probs(query_layer, key_layer):
    micro_count, seq_len, width = query_layer.shape
    head_count = width // HEAD_DIM
    query_heads = query_layer.astype(jnp.float32).reshape(micro_count, seq_len, head_count, HEAD_DIM)
    key_heads = key_layer.astype(jnp.float32).reshape(micro_count, seq_len, head_count, HEAD_DIM)
    scores = jnp.einsum('mihd,mjhd->mhij', query_heads, key_heads) / jnp.sqrt(jnp.float32(HEAD_DIM))
    rows = jnp.arange(seq_len)
    causal = rows[:, None] >= rows[None, :]
    scores = jnp.where(causal[None, None], scores, jnp.float32(-1e+30))
    highest = lax.optimization_barrier(jnp.max(scores, axis=-1, keepdims=True))
    expo = jnp.exp(scores - highest)
    return (expo / lax.optimization_barrier(jnp.sum(expo, axis=-1, keepdims=True))).astype(jnp.bfloat16)

def reference(cotangent, inputs, queries, keys, context, value_weight, out_weight):
    micro_count, seq_len, width = cotangent.shape
    head_count = width // HEAD_DIM
    upper = cotangent
    grads_list = []
    value_list = []
    out_list = []
    for layer in range(LAYERS - 1, -1, -1):
        upper_flat = upper.reshape(micro_count * seq_len, width)
        ctx_grad = jnp.dot(upper_flat.astype(jnp.float32), out_weight[layer].T.astype(jnp.float32), preferred_element_type=jnp.float32).astype(jnp.bfloat16)
        attention = attention_probs(queries[layer], keys[layer])
        ctx_heads = ctx_grad.reshape(micro_count, seq_len, head_count, HEAD_DIM).astype(jnp.float32)
        value_grad = jnp.einsum('mhij,mihd->mjhd', attention.astype(jnp.float32), ctx_heads)
        value_grad = value_grad.reshape(micro_count * seq_len, width).astype(jnp.bfloat16)
        branch = jnp.dot(value_grad.astype(jnp.float32), value_weight[layer].T.astype(jnp.float32), preferred_element_type=jnp.float32)
        lower = (upper_flat.astype(jnp.float32) + branch).astype(jnp.bfloat16)
        context_flat = context[layer].reshape(micro_count * seq_len, width)
        out_grad = jnp.dot(context_flat.T.astype(jnp.float32), upper_flat.astype(jnp.float32), preferred_element_type=jnp.float32).astype(jnp.bfloat16)
        input_flat = inputs[layer].reshape(micro_count * seq_len, width)
        value_wgrad = jnp.dot(input_flat.T.astype(jnp.float32), value_grad.astype(jnp.float32), preferred_element_type=jnp.float32).astype(jnp.bfloat16)
        upper = lower.reshape(micro_count, seq_len, width)
        grads_list.append(upper)
        value_list.append(value_wgrad)
        out_list.append(out_grad)
    grads_list = grads_list[::-1]
    value_list = value_list[::-1]
    out_list = out_list[::-1]
    return (jnp.stack(grads_list), jnp.stack(value_list), jnp.stack(out_list))
```

```python
import functools

import jax
import jax.numpy as jnp
from jax import lax
from jax.experimental import pallas as pl
from jax.experimental.pallas import tpu as pltpu
from jax.sharding import PartitionSpec as P

HEAD_DIM = 128
MIB = 1 << 20
F32 = jnp.float32
BF16 = jnp.bfloat16


def vmem():
    return pl.BlockSpec(memory_space=pltpu.VMEM)


def smem():
    return pl.BlockSpec(memory_space=pltpu.SMEM)


def params(mib):
    return pltpu.CompilerParams(vmem_limit_bytes=mib * MIB)


def cost(flops, moved):
    return pl.CostEstimate(flops=flops, bytes_accessed=moved, transcendentals=0)


def across(array, axis, flip):
    count = lax.axis_size(axis)
    return lax.ppermute(array, axis, [(i, i ^ flip) for i in range(count)])


def below(array, giver, flip):
    sections, tensors = lax.axis_size("section"), lax.axis_size("tensor")
    pairs = []
    for s in range(sections):
        peer = s - 1 if (s - giver) % 2 == 0 else s + 1
        if not 0 <= peer < sections:
            peer = s
        for t in range(tensors):
            pairs.append((s * tensors + t, peer * tensors + (t ^ flip)))
    return lax.ppermute(array, ("section", "tensor"), pairs)


def probs_kernel(order_ref, q_ref, k_ref, mask_ref, *out_refs):
    seq = q_ref.shape[1]
    heads = q_ref.shape[2] // HEAD_DIM
    half = heads // 2
    blocks = order_ref.shape[0]
    rows = seq // blocks
    causal = mask_ref[...] > 0
    for m, out_ref in enumerate(out_refs):
        starts = [pl.multiple_of(order_ref[b] * rows, rows) for b in range(blocks)]
        q = jnp.concatenate([q_ref[m, pl.ds(s, rows), :] for s in starts], axis=0)
        k = jnp.concatenate([k_ref[m, pl.ds(s, rows), :] for s in starts], axis=0)
        for h in range(heads):
            cols = slice(h * HEAD_DIM, (h + 1) * HEAD_DIM)
            scores = lax.dot_general(
                q[:, cols], k[:, cols], (((1,), (1,)), ((), ())), preferred_element_type=F32
            )
            scores = scores / jnp.sqrt(F32(HEAD_DIM))
            scores = jnp.where(causal, scores, F32(-1e30))
            expo = jnp.exp(scores - jnp.max(scores, axis=-1, keepdims=True))
            probs = (expo / jnp.sum(expo, axis=-1, keepdims=True)).astype(BF16)
            none = jnp.zeros((seq, seq), BF16)
            pair = [probs, none] if h < half else [none, probs]
            out_ref[h, :, :] = jnp.concatenate(pair, axis=0)


def attention_probs(order, queries, keys, mask):
    micro, seq, cols = queries.shape
    heads = cols // HEAD_DIM
    return pl.pallas_call(
        probs_kernel,
        out_shape=[jax.ShapeDtypeStruct((heads, 2 * seq, seq), BF16)] * micro,
        in_specs=[smem(), vmem(), vmem(), vmem()],
        out_specs=[vmem()] * micro,
        compiler_params=params(8),
        cost_estimate=cost(4 * micro * seq * seq * cols, 4 * micro * seq * cols),
        name="probs",
    )(order, queries, keys, mask)


def ctx_matmul(weight_ref, upper, part_ref):
    half = weight_ref.shape[0] // 2
    dims = (((1,), (1,)), ((), ()))
    step = half // 2
    for r in range(0, half, step):
        low = lax.dot_general(weight_ref[r : r + step, :], upper, dims, preferred_element_type=F32)
        high = lax.dot_general(
            weight_ref[half + r : half + r + step, :], upper, dims, preferred_element_type=F32
        )
        part_ref[r : r + step, :] = jnp.concatenate([low, high], axis=1).astype(BF16)


def first_kernel(*refs):
    blocks = refs[:-3]
    weight_ref, part_ref, upper_ref = refs[-3:]
    upper_ref[...] = jnp.concatenate([b[...] for b in blocks], axis=0)
    ctx_matmul(weight_ref, upper_ref[...], part_ref)


def next_kernel(rows, take_ref, *refs):
    near, far = refs[: (len(refs) - 4) // 2], refs[(len(refs) - 4) // 2 : -4]
    prev_ref, weight_ref, part_ref, upper_ref = refs[-4:]
    take = take_ref[0] > 0
    count = len(near)
    for side, group in enumerate((near, far)):
        for b in range(count):
            total = None
            for d, ref in enumerate(group):
                at = (b ^ d) * rows
                term = ref[at : at + rows, :].astype(F32)
                total = term if total is None else total + term
            at = (side * count + b) * rows
            old = prev_ref[at : at + rows, :]
            upper_ref[at : at + rows, :] = jnp.where(take, total, old.astype(F32)).astype(BF16)
    ctx_matmul(weight_ref, upper_ref[...], part_ref)


def ctx_call(kernel, specs, operands, tokens, weight, name):
    cols, width = weight.shape
    return pl.pallas_call(
        kernel,
        out_shape=[
            jax.ShapeDtypeStruct((cols // 2, 2 * tokens), BF16),
            jax.ShapeDtypeStruct((tokens, width), BF16),
        ],
        in_specs=specs,
        out_specs=[vmem(), vmem()],
        compiler_params=params(20),
        cost_estimate=cost(4 * tokens * cols * width, 2 * cols * width),
        name=name,
    )(*operands)


def branch_kernel(terms, *refs):
    parts, (probs_ref, weight_ref) = refs[:terms], refs[terms : terms + 2]
    keep_ref, send_ref, grad_ref = refs[terms + 2 :]
    tokens = probs_ref.shape[2]
    heads = probs_ref.shape[0]
    half = heads // 2
    packed = parts[0][...].astype(F32)
    for ref in parts[1:]:
        packed = packed + ref[...].astype(F32)
    packed = packed.astype(BF16)
    for h in range(heads):
        row = (h % half) * HEAD_DIM
        grad = jnp.dot(
            packed[row : row + HEAD_DIM, :], probs_ref[h], preferred_element_type=F32
        )
        grad_ref[h * HEAD_DIM : (h + 1) * HEAD_DIM, :] = grad.astype(BF16)
    grads = grad_ref[...]
    width = weight_ref.shape[0]
    step = min(width, 768)
    for r in range(0, width, step):
        out = jnp.dot(weight_ref[r : r + step, :], grads, preferred_element_type=F32)
        out = out.T.astype(BF16)
        keep_ref[:, r : r + step] = out[: tokens // 2]
        send_ref[:, r : r + step] = out[tokens // 2 :]


def branch(parts, probs, weight):
    width, cols = weight.shape
    tokens = probs.shape[2]
    half = jax.ShapeDtypeStruct((tokens // 2, width), BF16)
    return pl.pallas_call(
        functools.partial(branch_kernel, len(parts)),
        out_shape=[half, half, jax.ShapeDtypeStruct((cols, tokens), BF16)],
        in_specs=[vmem()] * (len(parts) + 2),
        out_specs=[vmem()] * 3,
        compiler_params=params(20),
        cost_estimate=cost(4 * tokens * cols * width, 2 * cols * width),
        name="branch",
    )(*parts, probs, weight)


def pair_kernel(rows, keep_ref, got_ref, upper_ref, out_ref):
    out = keep_ref[...].astype(F32) + got_ref[...].astype(F32)
    out_ref[:rows, :] = (out[:rows] + upper_ref[:rows, :].astype(F32)).astype(BF16)
    if out.shape[0] > rows:
        out_ref[rows:, :] = out[rows:].astype(BF16)


def pair_sum(keep, got, upper, rows):
    return pl.pallas_call(
        functools.partial(pair_kernel, rows),
        out_shape=jax.ShapeDtypeStruct(keep.shape, BF16),
        in_specs=[vmem()] * 3,
        out_specs=vmem(),
        compiler_params=params(4),
        cost_estimate=cost(keep.size, 6 * keep.size),
        name="pair",
    )(keep, got, upper)


def out_grad_kernel(order_ref, ctx_ref, *refs):
    uppers, out_ref, scratch = refs[:-2], refs[-2], refs[-1]
    tokens = uppers[0].shape[0]
    blocks = order_ref.shape[0]
    rows = tokens // blocks

    @pl.when(pl.program_id(0) == 0)
    def _():
        for m, ref in enumerate(uppers):
            for b in range(blocks):
                at = pl.multiple_of(m * tokens + order_ref[b] * rows, rows)
                scratch[pl.ds(at, rows), :] = ref[b * rows : (b + 1) * rows, :]

    out_ref[...] = lax.dot_general(
        ctx_ref[...], scratch[...], (((0,), (0,)), ((), ())), preferred_element_type=F32
    ).astype(BF16)


def out_grad(order, context, uppers, step):
    total, cols = context.shape
    width = uppers[0].shape[1]
    return pl.pallas_call(
        out_grad_kernel,
        grid=(cols // step,),
        out_shape=jax.ShapeDtypeStruct((cols, width), BF16),
        in_specs=[smem(), pl.BlockSpec((total, step), lambda i: (0, i))] + [vmem()] * len(uppers),
        out_specs=pl.BlockSpec((step, width), lambda i: (i, 0)),
        scratch_shapes=[pltpu.VMEM((total, width), BF16)],
        compiler_params=params(12),
        cost_estimate=cost(2 * total * cols * width, 2 * cols * width),
        name="out_grad",
    )(order, context, *uppers)


def value_grad_kernel(micro, *refs):
    blocks, grads, out_ref, rhs = refs[: -micro - 2], refs[-micro - 2 : -2], refs[-2], refs[-1]

    @pl.when(pl.program_id(0) == 0)
    def _():
        rhs[...] = jnp.concatenate([g[...] for g in grads], axis=1)

    lhs = jnp.concatenate([b[m] for m in range(micro) for b in blocks], axis=0)
    out_ref[...] = lax.dot_general(
        lhs, rhs[...], (((0,), (1,)), ((), ())), preferred_element_type=F32
    ).astype(BF16)


def value_weight_grad(blocks, grads, step):
    micro, rows, width = blocks[0].shape
    cols, tokens = grads[0].shape
    return pl.pallas_call(
        functools.partial(value_grad_kernel, micro),
        grid=(width // step,),
        out_shape=jax.ShapeDtypeStruct((width, cols), BF16),
        in_specs=[pl.BlockSpec((micro, rows, step), lambda i: (0, 0, i))] * len(blocks)
        + [vmem()] * micro,
        out_specs=pl.BlockSpec((step, cols), lambda i: (i, 0)),
        scratch_shapes=[pltpu.VMEM((cols, micro * tokens), BF16)],
        compiler_params=params(12),
        cost_estimate=cost(2 * micro * tokens * cols * width, 2 * cols * width),
        name="value_weight_grad",
    )(*blocks, *grads)


def per_device(cotangent, inputs, queries, keys, context, value_weight, out_weight):
    sections = lax.axis_size("section")
    place = lax.axis_index("section")
    tensors = lax.axis_size("tensor")
    here = lax.axis_index("tensor")
    replicas = lax.axis_size("dp")
    micro, rows, width = cotangent.shape
    seq = queries.shape[2]
    cols = queries.shape[3]
    flips = list(range(0, tensors, 2)) + list(range(1, tensors, 2))
    order = here ^ jnp.array(flips, jnp.int32)
    token = jnp.repeat(order, rows, total_repeat_length=seq) * rows + jnp.arange(seq) % rows
    mask = (token[:, None] >= token[None, :]).astype(jnp.int32)
    value_proj, out_proj = value_weight[0], out_weight[0]

    def gathered(block):
        own = {0: block}
        for f in range(2, tensors, 2):
            own[f] = across(block, "tensor", f)
        for f in range(0, tensors, 2):
            own[f + 1] = across(own[f], "tensor", 1)
        return [own[f] for f in flips]

    probs = attention_probs(order, queries[0], keys[0], mask)

    parts, uppers, grads, sums = [None] * micro, [None] * micro, [None] * micro, [None] * micro
    for m in range(micro):
        blocks = gathered(cotangent[m])
        parts[m], uppers[m] = ctx_call(
            first_kernel, [vmem()] * (len(blocks) + 1), (*blocks, out_proj), seq, out_proj, "first"
        )
    in_blocks = gathered(inputs[0])
    for stage in range(sections):
        for m in range(micro):
            heard = [across(parts[m], "dp", d) for d in range(1, replicas)]
            keep, send, grads[m] = branch([parts[m], *heard], probs[m], value_proj)
            got = across(send, "tensor", 1)
            sums[m] = pair_sum(keep, got, uppers[m], rows)
        if stage == sections - 1:
            break
        take = (place == sections - 2 - stage).astype(jnp.int32).reshape(1)
        for m in range(micro):
            near = [below(sums[m], sections - 1 - stage, f) for f in range(0, tensors, 2)]
            far = [across(n, "tensor", 1) for n in near]
            specs = [smem()] + [vmem()] * (len(near) + len(far) + 2)
            parts[m], uppers[m] = ctx_call(
                functools.partial(next_kernel, rows),
                specs,
                (take, *near, *far, uppers[m], out_proj),
                seq,
                out_proj,
                "next",
            )
    fresh = []
    for m in range(micro):
        total = sums[m][:rows].astype(F32)
        for b in range(1, tensors // 2):
            total = total + across(sums[m][b * rows : (b + 1) * rows], "tensor", 2 * b).astype(F32)
        fresh.append(total.astype(BF16))
    out_w = out_grad(order, context[0].reshape(micro * seq, cols), uppers, 256)
    value_w = value_weight_grad(in_blocks, grads, 256)
    return (jnp.stack(fresh)[None], value_w[None], out_w[None])


def solution(mesh):
    placed = (
        P(None, "tensor", "dp"),
        P("section", None, "tensor", "dp"),
        P("section", None, None, "tensor"),
        P("section", None, None, "tensor"),
        P("section", None, None, "tensor"),
        P("section", "dp", "tensor"),
        P("section", "tensor", "dp"),
    )
    return jax.shard_map(
        per_device,
        mesh=mesh,
        in_specs=placed,
        out_specs=(
            P("section", None, "tensor", "dp"),
            P("section", "dp", "tensor"),
            P("section", "tensor", "dp"),
        ),
        check_vma=False,
    )
```

```python
import functools

import jax
import jax.numpy as jnp
from jax import lax
from jax.experimental import pallas as pl
from jax.experimental.pallas import tpu as pltpu
from jax.sharding import PartitionSpec as P


HEAD_DIM = 128
MIB = 1 << 20
F32 = jnp.float32
BF16 = jnp.bfloat16


def vmem():
    return pl.BlockSpec(memory_space=pltpu.VMEM)


def params(mib):
    return pltpu.CompilerParams(vmem_limit_bytes=mib * MIB)


def cost(flops, moved):
    return pl.CostEstimate(flops=flops, bytes_accessed=moved, transcendentals=0)


def run(kernel, outs, operands, after, flops, moved):
    count = len(operands)

    def body(*refs):
        kernel(*refs[:count], *refs[count + len(after) :])

    return pl.pallas_call(
        body,
        out_shape=[jax.ShapeDtypeStruct(*out) for out in outs],
        in_specs=[vmem()] * (count + len(after)),
        out_specs=[vmem()] * len(outs),
        compiler_params=params(4),
        cost_estimate=cost(flops, moved),
    )(*operands, *after)


def across(array, axis, flip):
    count = lax.axis_size(axis)
    return lax.ppermute(array, axis, [(i, i ^ flip) for i in range(count)])


def below(array, giver, flip):
    sections, tensors = lax.axis_size("section"), lax.axis_size("tensor")
    pairs = []
    for s in range(sections):
        peer = s - 1 if (s - giver) % 2 == 0 else s + 1
        if not 0 <= peer < sections:
            peer = s
        for t in range(tensors):
            pairs.append((s * tensors + t, peer * tensors + (t ^ flip)))
    return lax.ppermute(array, ("section", "tensor"), pairs)


def token_order(tensors):
    here = lax.axis_index("tensor")
    return [here ^ f for f in [*range(0, tensors, 2), *range(1, tensors, 2)]]


def probs_kernel(tensors, q_ref, k_ref, *out_refs):
    seq = q_ref.shape[1]
    heads = q_ref.shape[2] // HEAD_DIM
    half = heads // 2
    rows = seq // tensors
    order = token_order(tensors)
    starts = [pl.multiple_of(block * rows, rows) for block in order]
    down = lax.broadcasted_iota(jnp.int32, (seq, seq), 0)
    along = lax.broadcasted_iota(jnp.int32, (seq, seq), 1)
    query_at, key_at = down % rows, along % rows
    for b, start in enumerate(starts):
        query_at = query_at + jnp.where(down // rows == b, start, 0)
        key_at = key_at + jnp.where(along // rows == b, start, 0)
    causal = query_at >= key_at
    for m, out_ref in enumerate(out_refs):
        q = jnp.concatenate([q_ref[m, pl.ds(s, rows), :] for s in starts], axis=0)
        k = jnp.concatenate([k_ref[m, pl.ds(s, rows), :] for s in starts], axis=0)
        for h in range(heads):
            cols = slice(h * HEAD_DIM, (h + 1) * HEAD_DIM)
            scores = lax.dot_general(
                q[:, cols], k[:, cols], (((1,), (1,)), ((), ())), preferred_element_type=F32
            )
            scores = scores / jnp.sqrt(F32(HEAD_DIM))
            scores = jnp.where(causal, scores, F32(-1e30))
            expo = jnp.exp(scores - jnp.max(scores, axis=-1, keepdims=True))
            probs = (expo / jnp.sum(expo, axis=-1, keepdims=True)).astype(BF16)
            none = jnp.zeros((seq, seq), BF16)
            pair = [probs, none] if h < half else [none, probs]
            out_ref[h, :, :] = jnp.concatenate(pair, axis=0)


def attention_probs(queries, keys, tensors):
    micro, seq, cols = queries.shape
    outs = [((cols // HEAD_DIM, 2 * seq, seq), BF16)] * micro
    flops = 4 * micro * seq * seq * cols
    kernel = functools.partial(probs_kernel, tensors)
    return run(kernel, outs, [queries, keys], [], flops, 4 * queries.size)


def ctx_matmul(weight_ref, upper, part_ref):
    half = weight_ref.shape[0] // 2
    step = min(half, 384)
    dims = (((1,), (1,)), ((), ()))
    for at in range(0, half, step):
        low, high = (
            lax.dot_general(
                weight_ref[at + off : at + off + step, :], upper, dims, preferred_element_type=F32
            )
            for off in (0, half)
        )
        part_ref[at : at + step, :] = jnp.concatenate([low, high], axis=1).astype(BF16)


def first_kernel(*refs):
    blocks = refs[:-3]
    weight_ref, part_ref, upper_ref = refs[-3:]
    upper_ref[...] = jnp.concatenate([b[...] for b in blocks], axis=0)
    ctx_matmul(weight_ref, upper_ref[...], part_ref)


def next_kernel(rows, taker, *refs):
    blocks = refs[:-4]
    prev_ref, weight_ref, part_ref, upper_ref = refs[-4:]
    take = lax.axis_index("section") == taker
    for b, ref in enumerate(blocks):
        at = slice(b * rows, (b + 1) * rows)
        upper_ref[at, :] = jnp.where(take, ref[...], prev_ref[at, :])
    ctx_matmul(weight_ref, upper_ref[...], part_ref)


def ctx_call(kernel, operands, tokens, weight, after):
    cols, width = weight.shape
    outs = [((cols // 2, 2 * tokens), BF16), ((tokens, width), BF16)]
    flops = 2 * tokens * cols * width
    return run(kernel, outs, [*operands, weight], after, flops, 2 * weight.size)


def branch_kernel(terms, *refs):
    parts, (probs_ref, weight_ref) = refs[:terms], refs[terms : terms + 2]
    keep_ref, send_ref, grad_ref = refs[-3:]
    tokens = probs_ref.shape[2]
    heads = probs_ref.shape[0]
    half = heads // 2
    packed = parts[0][...].astype(F32)
    for ref in parts[1:]:
        packed = packed + ref[...].astype(F32)
    packed = packed.astype(BF16)
    for h in range(heads):
        row = (h % half) * HEAD_DIM
        grad = jnp.dot(
            packed[row : row + HEAD_DIM, :], probs_ref[h], preferred_element_type=F32
        )
        grad_ref[h * HEAD_DIM : (h + 1) * HEAD_DIM, :] = grad.astype(BF16)
    grads = grad_ref[...]
    width = weight_ref.shape[0]
    step = min(width, 768)
    for at in range(0, width, step):
        out = jnp.dot(weight_ref[at : at + step, :], grads, preferred_element_type=F32)
        out = out.T.astype(BF16)
        keep_ref[:, at : at + step] = out[: tokens // 2]
        send_ref[:, at : at + step] = out[tokens // 2 :]


def branch(parts, probs, weight, after):
    width, cols = weight.shape
    tokens = probs.shape[2]
    half = ((tokens // 2, width), BF16)
    outs = [half, half, ((cols, tokens), BF16)]
    kernel = functools.partial(branch_kernel, len(parts))
    flops = 2 * tokens * cols * width
    return run(kernel, outs, [*parts, probs, weight], after, flops, 2 * weight.size)


def pair_kernel(rows, keep_ref, got_ref, mine_ref, *away_refs):
    out = keep_ref[...].astype(F32) + got_ref[...].astype(F32)
    mine_ref[...] = out[:rows]
    for b, ref in enumerate(away_refs):
        ref[...] = out[(b + 1) * rows : (b + 2) * rows].astype(BF16)


def pair_sum(keep, got, rows, after):
    total, width = keep.shape
    outs = [((rows, width), F32)] + [((rows, width), BF16)] * (total // rows - 1)
    kernel = functools.partial(pair_kernel, rows)
    return run(kernel, outs, [keep, got], after, keep.size, 6 * keep.size)


def fresh_kernel(*refs):
    mine_ref, upper_ref, out_ref = refs[0], refs[-2], refs[-1]
    total = mine_ref[...]
    for ref in refs[1:-2]:
        total = total + ref[...].astype(F32)
    rows = mine_ref.shape[0]
    out_ref[...] = (total + upper_ref[:rows, :].astype(F32)).astype(BF16)


def fresh_rows(mine, heard, upper, after):
    operands = [mine, *heard, upper]
    outs = [(mine.shape, BF16)]
    return run(fresh_kernel, outs, operands, after, mine.size, 6 * mine.size)[0]


def hold_kernel(src_ref, out_ref, sems):
    parts = sems.shape[0]
    rows = src_ref.shape[0] // parts
    copies = [
        pltpu.make_async_copy(
            src_ref.at[pl.ds(i * rows, rows), :], out_ref.at[pl.ds(i * rows, rows), :], sems.at[i]
        )
        for i in range(parts)
    ]
    for copy in copies:
        copy.start()
    for copy in copies:
        copy.wait()


def held(array):
    return pl.pallas_call(
        hold_kernel,
        out_shape=jax.ShapeDtypeStruct(array.shape, array.dtype),
        in_specs=[pl.BlockSpec(memory_space=pltpu.HBM)],
        out_specs=vmem(),
        scratch_shapes=[pltpu.SemaphoreType.DMA((4,))],
        compiler_params=params(4),
        cost_estimate=cost(array.size, 2 * array.size),
        name="held",
    )(pltpu.with_memory_space_constraint(array, pltpu.HBM))


def stream_product(lhs_of, rhs, out_ref, buf, sems):
    count = sems.shape[0]
    step = buf.shape[0] // count

    def copy(i):
        rows = pl.ds(pl.multiple_of(i * step, step), step)
        return pltpu.make_async_copy(buf.at[rows, :], out_ref.at[rows, :], sems.at[i])

    @pl.loop(0, count, unroll=2)
    def _(i):
        rows = pl.ds(pl.multiple_of(i * step, step), step)
        product = jnp.dot(lhs_of(rows).T, rhs, preferred_element_type=F32)
        buf[rows, :] = product.astype(BF16)
        copy(i).start()

    @pl.loop(0, count)
    def _(i):
        copy(i).wait()


def out_grad_kernel(tensors, ctx_ref, *refs):
    uppers, (out_ref, buf, sems, rhs) = refs[:-4], refs[-4:]
    tokens = uppers[0].shape[0]
    rows = tokens // tensors
    for m, ref in enumerate(uppers):
        for b, block in enumerate(token_order(tensors)):
            at = pl.multiple_of(m * tokens + block * rows, rows)
            rhs[pl.ds(at, rows), :] = ref[b * rows : (b + 1) * rows, :]
    stream_product(lambda at: ctx_ref[:, at], rhs[...], out_ref, buf, sems)


def value_grad_kernel(micro, *refs):
    blocks, grads = refs[: -micro - 4], refs[-micro - 4 : -4]
    out_ref, buf, sems, rhs = refs[-4:]
    tokens = grads[0].shape[1]
    for m, ref in enumerate(grads):
        rhs[m * tokens : (m + 1) * tokens, :] = ref[...].T

    def lhs_of(at):
        return jnp.concatenate([b[m, :, at] for m in range(micro) for b in blocks], axis=0)

    stream_product(lhs_of, rhs[...], out_ref, buf, sems)


def weight_grad(kernel, operands, shape, tokens):
    rows, cols = shape
    step = min(rows, 256)
    return pl.pallas_call(
        kernel,
        out_shape=jax.ShapeDtypeStruct(shape, BF16),
        in_specs=[vmem()] * len(operands),
        out_specs=pl.BlockSpec(memory_space=pltpu.HBM),
        scratch_shapes=[
            pltpu.VMEM(shape, BF16),
            pltpu.SemaphoreType.DMA((rows // step,)),
            pltpu.VMEM((tokens, cols), BF16),
        ],
        compiler_params=params(20),
        cost_estimate=cost(2 * tokens * rows * cols, 2 * rows * cols),
    )(*operands)


def per_device(cotangent, inputs, queries, keys, context, value_weight, out_weight):
    sections = lax.axis_size("section")
    tensors = lax.axis_size("tensor")
    replicas = lax.axis_size("dp")
    micro, rows, width = cotangent.shape
    seq, cols = queries.shape[2:]
    value_proj = value_weight[0]
    turns = range(0, tensors, 2)

    def both_cores(near):
        return [*near, *(across(n, "tensor", 1) for n in near)]

    def gathered(block):
        near = [block] + [across(block, "tensor", f) for f in turns[1:]]
        return both_cores(near)

    first = []
    for m in range(micro):
        first.append(gathered(cotangent[m]))
    probs = attention_probs(queries[0], keys[0], tensors)
    out_proj = held(out_weight[0])
    parts, uppers, grads, fresh = [None] * micro, [None] * micro, [None] * micro, [None] * micro
    last = list(probs[:1])
    for m in range(micro):
        parts[m], uppers[m] = ctx_call(first_kernel, first[m], seq, out_proj, last)
        last = [parts[m]]
    in_blocks = gathered(inputs[0])
    for stage in range(sections):
        giver = sections - 1 - stage
        mine, away = [None] * micro, [None] * micro
        for m in range(micro + 1):
            if m < micro:
                heard = [across(parts[m], "dp", d) for d in range(1, replicas)]
                keep, send, grads[m] = branch(
                    [parts[m], *heard], probs[m], value_proj, last
                )
                last = [send]
            if m > 0:
                heard = [across(a, "tensor", f) for a, f in zip(away[m - 1], turns[1:])]
                fresh[m - 1] = fresh_rows(mine[m - 1], heard, uppers[m - 1], last)
                last = [fresh[m - 1]]
            if m < micro:
                mine[m], *away[m] = pair_sum(keep, across(send, "tensor", 1), rows, last)
                last = [mine[m]]
        if stage == sections - 1:
            break
        for m in range(micro):
            blocks = both_cores([below(fresh[m], giver, f) for f in turns])
            kernel = functools.partial(next_kernel, rows, giver - 1)
            parts[m], uppers[m] = ctx_call(kernel, [*blocks, uppers[m]], seq, out_proj, last)
            last = [parts[m]]
    out_w = weight_grad(
        functools.partial(out_grad_kernel, tensors),
        [context[0].reshape(micro * seq, cols), *uppers],
        (cols, width),
        micro * seq,
    )
    value_w = weight_grad(
        functools.partial(value_grad_kernel, micro),
        [*in_blocks, *grads],
        (width, cols),
        micro * seq,
    )
    return (jnp.stack(fresh)[None], value_w[None], out_w[None])


def solution(mesh):
    placed = (
        P(None, "tensor", "dp"),
        P("section", None, "tensor", "dp"),
        P("section", None, None, "tensor"),
        P("section", None, None, "tensor"),
        P("section", None, None, "tensor"),
        P("section", "dp", "tensor"),
        P("section", "tensor", "dp"),
    )
    return jax.shard_map(
        per_device,
        mesh=mesh,
        in_specs=placed,
        out_specs=(
            P("section", None, "tensor", "dp"),
            P("section", "dp", "tensor"),
            P("section", "tensor", "dp"),
        ),
        check_vma=False,
    )
```

```python
import functools

import jax
import jax.numpy as jnp
from jax import lax
from jax.experimental import pallas as pl
from jax.experimental.pallas import tpu as pltpu
from jax.sharding import PartitionSpec as P


HEAD_DIM = 128
MIB = 1 << 20
F32 = jnp.float32
BF16 = jnp.bfloat16


def vmem():
    return pl.BlockSpec(memory_space=pltpu.VMEM)


def params(mib):
    return pltpu.CompilerParams(vmem_limit_bytes=mib * MIB)


def cost(flops, moved):
    return pl.CostEstimate(flops=flops, bytes_accessed=moved, transcendentals=0)


def run(kernel, outs, operands, after, flops, moved):
    count = len(operands)

    def body(*refs):
        kernel(*refs[:count], *refs[count + len(after) :])

    return pl.pallas_call(
        body,
        out_shape=[jax.ShapeDtypeStruct(*out) for out in outs],
        in_specs=[vmem()] * (count + len(after)),
        out_specs=[vmem()] * len(outs),
        compiler_params=params(4),
        cost_estimate=cost(flops, moved),
    )(*operands, *after)


def across(array, axis, flip):
    count = lax.axis_size(axis)
    return lax.ppermute(array, axis, [(i, i ^ flip) for i in range(count)])


def below(array, giver, flip):
    sections, tensors = lax.axis_size("section"), lax.axis_size("tensor")
    pairs = []
    for s in range(sections):
        peer = s - 1 if (s - giver) % 2 == 0 else s + 1
        if not 0 <= peer < sections:
            peer = s
        for t in range(tensors):
            pairs.append((s * tensors + t, peer * tensors + (t ^ flip)))
    return lax.ppermute(array, ("section", "tensor"), pairs)


def core_side():
    return lax.rem(lax.axis_index("tensor"), 2)


def token_order(tensors):
    base = lax.axis_index("tensor") - core_side()
    return [base ^ j for j in range(tensors)]


def part(index, size):
    return pl.ds(pl.multiple_of(index * size, size), size)


def probs_kernel(tensors, q_ref, k_ref, *out_refs):
    seq = q_ref.shape[1]
    heads = q_ref.shape[2] // HEAD_DIM
    half = heads // 2
    rows = seq // tensors
    order = token_order(tensors)
    starts = [pl.multiple_of(block * rows, rows) for block in order]
    down = lax.broadcasted_iota(jnp.int32, (seq, seq), 0)
    along = lax.broadcasted_iota(jnp.int32, (seq, seq), 1)
    query_at, key_at = down % rows, along % rows
    for b, start in enumerate(starts):
        query_at = query_at + jnp.where(down // rows == b, start, 0)
        key_at = key_at + jnp.where(along // rows == b, start, 0)
    causal = query_at >= key_at
    for m, out_ref in enumerate(out_refs):
        q = jnp.concatenate([q_ref[m, pl.ds(s, rows), :] for s in starts], axis=0)
        k = jnp.concatenate([k_ref[m, pl.ds(s, rows), :] for s in starts], axis=0)
        for h in range(heads):
            cols = slice(h * HEAD_DIM, (h + 1) * HEAD_DIM)
            scores = lax.dot_general(
                q[:, cols], k[:, cols], (((1,), (1,)), ((), ())), preferred_element_type=F32
            )
            scores = scores / jnp.sqrt(F32(HEAD_DIM))
            scores = jnp.where(causal, scores, F32(-1e30))
            expo = jnp.exp(scores - jnp.max(scores, axis=-1, keepdims=True))
            probs = (expo / jnp.sum(expo, axis=-1, keepdims=True)).astype(BF16)
            none = jnp.zeros((seq, seq), BF16)
            pair = [probs, none] if h < half else [none, probs]
            out_ref[h, :, :] = jnp.concatenate(pair, axis=0)


def attention_probs(queries, keys, tensors):
    micro, seq, cols = queries.shape
    outs = [((cols // HEAD_DIM, 2 * seq, seq), BF16)] * micro
    flops = 4 * micro * seq * seq * cols
    kernel = functools.partial(probs_kernel, tensors)
    return run(kernel, outs, [queries, keys], [], flops, 4 * queries.size)


def ctx_matmul(weight_ref, terms, start_ref, out_ref):
    half = weight_ref.shape[0] // 2
    step = min(half, 384)
    dims = (((1,), (1,)), ((), ()))
    for at in range(0, half, step):
        sides = []
        for off in (0, half):
            rows = slice(at + off, at + off + step)
            total = None
            for cols, upper in terms:
                term = lax.dot_general(
                    weight_ref[rows, cols], upper, dims, preferred_element_type=F32
                )
                total = term if total is None else total + term
            sides.append(total)
        out = jnp.concatenate(sides, axis=1)
        if start_ref is not None:
            out = out + start_ref[at : at + step, :]
        out_ref[at : at + step, :] = out.astype(out_ref.dtype)


def first_kernel(*refs):
    blocks, (weight_ref, part_ref, near_ref, far_ref) = refs[:-4], refs[-4:]
    side = core_side()
    rows, width = blocks[0].shape
    near, far = part(side, width // 2), part(1 - side, width // 2)
    for flip, ref in enumerate(blocks):
        at = part(side ^ flip, rows)
        near_ref[at, :] = ref[:, near]
        far_ref[at, :] = ref[:, far]
    ctx_matmul(weight_ref, [(near, near_ref[...]), (far, far_ref[...])], None, part_ref)


def take_turn(taker, blocks, prev_ref, upper_ref):
    take = lax.axis_index("section") == taker
    rows = blocks[0].shape[0]
    for b, ref in enumerate(blocks):
        at = slice(b * rows, (b + 1) * rows)
        upper_ref[at, :] = jnp.where(take, ref[...], prev_ref[at, :])


def near_kernel(taker, *refs):
    blocks, (prev_ref, weight_ref, start_ref, upper_ref) = refs[:-4], refs[-4:]
    take_turn(taker, blocks, prev_ref, upper_ref)
    cols = part(core_side(), upper_ref.shape[1])
    ctx_matmul(weight_ref, [(cols, upper_ref[...])], None, start_ref)


def far_kernel(taker, *refs):
    blocks, (prev_ref, start_ref, weight_ref, part_ref, upper_ref) = refs[:-5], refs[-5:]
    take_turn(taker, blocks, prev_ref, upper_ref)
    cols = part(1 - core_side(), upper_ref.shape[1])
    ctx_matmul(weight_ref, [(cols, upper_ref[...])], start_ref, part_ref)


def first_ctx(blocks, weight, tokens, after):
    cols, width = weight.shape
    side = ((tokens, width // 2), BF16)
    outs = [((cols // 2, 2 * tokens), BF16), side, side]
    flops = 2 * tokens * cols * width
    return run(first_kernel, outs, [*blocks, weight], after, flops, 2 * weight.size)


def half_ctx(taker, blocks, prev, start, weight, after):
    cols, tokens = weight.shape[0], prev.shape[0]
    kernel = functools.partial(near_kernel if start is None else far_kernel, taker)
    starts = [] if start is None else [start]
    outs = [((cols // 2, 2 * tokens), F32 if start is None else BF16), (prev.shape, BF16)]
    operands = [*blocks, prev, *starts, weight]
    return run(kernel, outs, operands, after, 2 * cols * prev.size, weight.size)


def value_grads(terms, probs_ref, grad_ref):
    half = probs_ref.shape[0] // 2
    packed = terms[0][...].astype(F32)
    for ref in terms[1:]:
        packed = packed + ref[...].astype(F32)
    packed = packed.astype(BF16)
    for h in range(2 * half):
        row = (h % half) * HEAD_DIM
        grad = jnp.dot(
            packed[row : row + HEAD_DIM, :], probs_ref[h], preferred_element_type=F32
        )
        grad_ref[h * HEAD_DIM : (h + 1) * HEAD_DIM, :] = grad.astype(BF16)


def branch_rows(weight_ref, first, count, grads):
    step = min(count, 768)
    for at in range(0, count, step):
        rows = pl.ds(pl.multiple_of(first * count + at, 128), step)
        out = jnp.dot(weight_ref[rows, :], grads, preferred_element_type=F32)
        yield slice(at, at + step), out.T


def send_kernel(*refs):
    terms, (probs_ref, weight_ref, send_ref, grad_ref) = refs[:-4], refs[-4:]
    value_grads(terms, probs_ref, grad_ref)
    half = send_ref.shape[1]
    for at, out in branch_rows(weight_ref, 1 - core_side(), half, grad_ref[...]):
        send_ref[:, at] = out.astype(BF16)


def keep_kernel(grad_ref, weight_ref, keep_ref):
    half = keep_ref.shape[1]
    for at, out in branch_rows(weight_ref, core_side(), half, grad_ref[...]):
        keep_ref[:, at] = out


def send_branch(terms, probs, weight, after):
    width, cols = weight.shape
    tokens = probs.shape[2]
    outs = [((tokens, width // 2), BF16), ((cols, tokens), BF16)]
    flops = tokens * cols * width
    return run(send_kernel, outs, [*terms, probs, weight], after, flops, weight.size)


def keep_branch(grads, weight, after):
    width, cols = weight.shape
    tokens = grads.shape[1]
    outs = [((tokens, width // 2), F32)]
    flops = tokens * cols * width
    return run(keep_kernel, outs, [grads, weight], after, flops, weight.size)[0]


def last_kernel(rows, *refs):
    terms, (probs_ref, weight_ref, keep_ref, send_ref, grad_ref) = refs[:-5], refs[-5:]
    value_grads(terms, probs_ref, grad_ref)
    low = core_side() == 0
    for at, out in branch_rows(weight_ref, 0, keep_ref.shape[1], grad_ref[...]):
        for b in range(keep_ref.shape[0] // rows):
            one = out[2 * b * rows : (2 * b + 1) * rows]
            two = out[(2 * b + 1) * rows : (2 * b + 2) * rows]
            keep_ref[b * rows : (b + 1) * rows, at] = jnp.where(low, one, two)
            send_ref[b * rows : (b + 1) * rows, at] = jnp.where(low, two, one).astype(BF16)


def last_branch(terms, probs, weight, rows, after):
    width, cols = weight.shape
    tokens = probs.shape[2]
    half = (tokens // 2, width)
    outs = [(half, F32), (half, BF16), ((cols, tokens), BF16)]
    kernel = functools.partial(last_kernel, rows)
    flops = 2 * tokens * cols * width
    return run(kernel, outs, [*terms, probs, weight], after, flops, 2 * weight.size)


def pair_kernel(keep_ref, got_ref, mine_ref, *away_refs):
    total = keep_ref[...] + got_ref[...].astype(F32)
    rows = mine_ref.shape[0]
    mine_ref[...] = total[:rows]
    for b, ref in enumerate(away_refs, 1):
        ref[...] = total[b * rows : (b + 1) * rows].astype(BF16)


def pair_sum(keep, got, chips, after):
    total, width = keep.shape
    shape = (total // chips, width)
    outs = [(shape, F32)] + [(shape, BF16)] * (chips - 1)
    return run(pair_kernel, outs, [keep, got], after, keep.size, 6 * keep.size)


def fresh_kernel(*refs):
    mine_ref, heard, (upper_ref, out_ref) = refs[0], refs[1:-2], refs[-2:]
    total = mine_ref[...]
    for ref in heard:
        total = total + ref[...].astype(F32)
    rows = mine_ref.shape[0]
    out_ref[...] = (total + upper_ref[:rows, :].astype(F32)).astype(BF16)


def fresh_rows(mine, heard, upper, after):
    operands = [mine, *heard, upper]
    outs = [(mine.shape, BF16)]
    return run(fresh_kernel, outs, operands, after, mine.size, 6 * mine.size)[0]


def result_kernel(micro, *refs):
    out_ref = refs[-1]
    rows, half = out_ref.shape[1], out_ref.shape[2] // 2
    each = (len(refs) - 1) // micro
    side = core_side()
    for m in range(micro):
        mine_ref, *heard, near_ref, far_ref = refs[m * each : (m + 1) * each]
        for upper_ref, cols in ((near_ref, part(side, half)), (far_ref, part(1 - side, half))):
            total = mine_ref[:, cols]
            for ref in heard:
                total = total + ref[:, cols].astype(F32)
            upper = upper_ref[part(side, rows), :].astype(F32)
            out_ref[m, :, cols] = (total + upper).astype(BF16)


def result_rows(mine, heard, uppers):
    micro, (rows, width) = len(mine), mine[0].shape
    operands = []
    for m in range(micro):
        operands += [mine[m], *heard[m], *uppers[m]]
    kernel = functools.partial(result_kernel, micro)
    size = micro * rows * width
    outs = [((micro, rows, width), BF16)]
    return run(kernel, outs, operands, [], size, 6 * size)[0]


def hold_kernel(src_ref, out_ref, sems):
    parts = sems.shape[0]
    rows = src_ref.shape[0] // parts
    copies = [
        pltpu.make_async_copy(
            src_ref.at[pl.ds(i * rows, rows), :], out_ref.at[pl.ds(i * rows, rows), :], sems.at[i]
        )
        for i in range(parts)
    ]
    for copy in copies:
        copy.start()
    for copy in copies:
        copy.wait()


def held(array):
    return pl.pallas_call(
        hold_kernel,
        out_shape=jax.ShapeDtypeStruct(array.shape, array.dtype),
        in_specs=[pl.BlockSpec(memory_space=pltpu.HBM)],
        out_specs=vmem(),
        scratch_shapes=[pltpu.SemaphoreType.DMA((8,))],
        compiler_params=params(4),
        cost_estimate=cost(array.size, 2 * array.size),
        name="held",
    )(pltpu.with_memory_space_constraint(array, pltpu.HBM))


def stream_product(lhs_of, rhs, out_ref, buf, sems):
    count = sems.shape[0]
    step = buf.shape[0] // count

    def copy(i):
        rows = pl.ds(pl.multiple_of(i * step, step), step)
        return pltpu.make_async_copy(buf.at[rows, :], out_ref.at[rows, :], sems.at[i])

    @pl.loop(0, count, unroll=2)
    def _(i):
        rows = pl.ds(pl.multiple_of(i * step, step), step)
        product = jnp.dot(lhs_of(rows).T, rhs, preferred_element_type=F32)
        buf[rows, :] = product.astype(BF16)
        copy(i).start()

    @pl.loop(0, count)
    def _(i):
        copy(i).wait()


def out_grad_kernel(tensors, ctx_ref, *refs):
    uppers, (out_ref, buf, sems, _, rhs) = refs[:-5], refs[-5:]
    tokens, half = uppers[0].shape
    rows = tokens // tensors
    sides = (core_side(), 1 - core_side())
    for i, ref in enumerate(uppers):
        for b, block in enumerate(token_order(tensors)):
            at = pl.multiple_of((i // 2) * tokens + block * rows, rows)
            rhs[pl.ds(at, rows), part(sides[i % 2], half)] = ref[b * rows : (b + 1) * rows, :]
    stream_product(lambda at: ctx_ref[:, at], rhs[...], out_ref, buf, sems)


def value_grad_kernel(micro, *refs):
    blocks, grads = refs[: -micro - 5], refs[-micro - 5 : -5]
    out_ref, buf, sems, lhs, rhs = refs[-5:]
    tokens = grads[0].shape[1]
    rows = tokens // len(blocks)
    for m, ref in enumerate(grads):
        rhs[m * tokens : (m + 1) * tokens, :] = ref[...].T
        for flip, block in enumerate(blocks):
            at = pl.multiple_of(m * tokens + (core_side() ^ flip) * rows, rows)
            lhs[pl.ds(at, rows), :] = block[m]
    stream_product(lambda at: lhs[:, at], rhs[...], out_ref, buf, sems)


def weight_grad(kernel, operands, shape, tokens):
    rows, cols = shape
    step = min(rows, 256)
    return pl.pallas_call(
        kernel,
        out_shape=jax.ShapeDtypeStruct(shape, BF16),
        in_specs=[vmem()] * len(operands),
        out_specs=pl.BlockSpec(memory_space=pltpu.HBM),
        scratch_shapes=[
            pltpu.VMEM(shape, BF16),
            pltpu.SemaphoreType.DMA((rows // step,)),
            pltpu.VMEM((tokens, rows), BF16),
            pltpu.VMEM((tokens, cols), BF16),
        ],
        compiler_params=params(20),
        cost_estimate=cost(2 * tokens * rows * cols, 2 * rows * cols),
    )(*operands)


def per_device(cotangent, inputs, queries, keys, context, value_weight, out_weight):
    sections = lax.axis_size("section")
    tensors = lax.axis_size("tensor")
    replicas = lax.axis_size("dp")
    micro, rows, width = cotangent.shape
    seq, cols = queries.shape[2:]
    value_proj = value_weight[0]
    turns = range(0, tensors, 2)

    def gathered(block):
        near = [block] + [across(block, "tensor", f) for f in turns[1:]]
        far = [across(n, "tensor", 1) for n in near]
        return [b for both in zip(near, far) for b in both]

    def each():
        return [None] * micro

    first = each()
    for m in range(micro):
        first[m] = gathered(cotangent[m])
    probs = attention_probs(queries[0], keys[0], tensors)
    out_proj = held(out_weight[0])
    parts, nears, fars, grads = each(), each(), each(), each()
    last = list(probs[:1])
    for m in range(micro):
        parts[m], nears[m], fars[m] = first_ctx(first[m], out_proj, seq, last)
        last = [parts[m]]
    in_blocks = gathered(inputs[0])
    for stage in range(sections):
        ending = stage == sections - 1
        mine, heard = each(), each()
        for m in range(micro):
            terms = [parts[m]] + [across(parts[m], "dp", d) for d in range(1, replicas)]
            if ending:
                keep, send, grads[m] = last_branch(terms, probs[m], value_proj, rows, last)
                got = across(send, "tensor", 1)
            else:
                send, grads[m] = send_branch(terms, probs[m], value_proj, last)
                got = across(send, "tensor", 1)
                keep = keep_branch(grads[m], value_proj, [send])
            mine[m], *away = pair_sum(keep, got, tensors // 2, [])
            last = [mine[m]]
            heard[m] = [across(a, "tensor", f) for a, f in zip(away, turns[1:])]
        if ending:
            break
        fresh = each()
        last = last + (in_blocks[2::2] if stage == 0 else in_blocks[1::2] if stage == 1 else [])
        for m in range(micro):
            fresh[m] = fresh_rows(mine[m], heard[m], nears[m], last)
            last = [fresh[m]]
        for m in range(micro):
            near = [below(fresh[m], sections - 1 - stage, f) for f in turns]
            far = [across(n, "tensor", 1) for n in near]
            taker = sections - 2 - stage
            start, nears[m] = half_ctx(taker, near, nears[m], None, out_proj, last)
            parts[m], fars[m] = half_ctx(taker, far, fars[m], start, out_proj, [])
            last = [parts[m]]
    uppers = list(zip(nears, fars))
    result = result_rows(mine, heard, uppers)
    out_w = weight_grad(
        functools.partial(out_grad_kernel, tensors),
        [context[0].reshape(micro * seq, cols), *(side for both in uppers for side in both)],
        (cols, width),
        micro * seq,
    )
    value_w = weight_grad(
        functools.partial(value_grad_kernel, micro),
        [*in_blocks, *grads],
        (width, cols),
        micro * seq,
    )
    return (result[None], value_w[None], out_w[None])


def solution(mesh):
    placed = (
        P(None, "tensor", "dp"),
        P("section", None, "tensor", "dp"),
        P("section", None, None, "tensor"),
        P("section", None, None, "tensor"),
        P("section", None, None, "tensor"),
        P("section", "dp", "tensor"),
        P("section", "tensor", "dp"),
    )
    return jax.shard_map(
        per_device,
        mesh=mesh,
        in_specs=placed,
        out_specs=(
            P("section", None, "tensor", "dp"),
            P("section", "dp", "tensor"),
            P("section", "tensor", "dp"),
        ),
        check_vma=False,
    )
```

```python
import functools

import jax
import jax.numpy as jnp
from jax import lax
from jax.experimental import pallas as pl
from jax.experimental.pallas import tpu as pltpu
from jax.sharding import PartitionSpec as P


HEAD_DIM = 128
MIB = 1 << 20
F32 = jnp.float32
BF16 = jnp.bfloat16


def vmem():
    return pl.BlockSpec(memory_space=pltpu.VMEM)


def params(mib):
    return pltpu.CompilerParams(vmem_limit_bytes=mib * MIB)


def cost(flops, moved):
    return pl.CostEstimate(flops=flops, bytes_accessed=moved, transcendentals=0)


def run(kernel, outs, operands, after, flops, moved):
    count = len(operands)

    def body(*refs):
        kernel(*refs[:count], *refs[count + len(after) :])

    return pl.pallas_call(
        body,
        out_shape=[jax.ShapeDtypeStruct(*out) for out in outs],
        in_specs=[vmem()] * (count + len(after)),
        out_specs=[vmem()] * len(outs),
        compiler_params=params(4),
        cost_estimate=cost(flops, moved),
    )(*operands, *after)


def across(array, axis, flip):
    count = lax.axis_size(axis)
    return lax.ppermute(array, axis, [(i, i ^ flip) for i in range(count)])


def below(array, giver):
    count = lax.axis_size("section")
    pairs = []
    for s in range(count):
        peer = s - 1 if (s - giver) % 2 == 0 else s + 1
        pairs.append((s, peer if 0 <= peer < count else s))
    return lax.ppermute(array, "section", pairs)


def core_side():
    return lax.rem(lax.axis_index("tensor"), 2)


def token_order(tensors):
    base = lax.axis_index("tensor") - core_side()
    return [base ^ j for j in range(tensors)]


def part(index, size):
    return pl.ds(pl.multiple_of(index * size, size), size)


def probs_kernel(tensors, q_ref, k_ref, *out_refs):
    seq = q_ref.shape[1]
    heads = q_ref.shape[2] // HEAD_DIM
    half = heads // 2
    rows = seq // tensors
    order = token_order(tensors)
    starts = [pl.multiple_of(block * rows, rows) for block in order]
    down = lax.broadcasted_iota(jnp.int32, (seq, seq), 0)
    along = lax.broadcasted_iota(jnp.int32, (seq, seq), 1)
    query_at, key_at = down % rows, along % rows
    for b, start in enumerate(starts):
        query_at = query_at + jnp.where(down // rows == b, start, 0)
        key_at = key_at + jnp.where(along // rows == b, start, 0)
    causal = query_at >= key_at
    for m, out_ref in enumerate(out_refs):
        q = jnp.concatenate([q_ref[m, pl.ds(s, rows), :] for s in starts], axis=0)
        k = jnp.concatenate([k_ref[m, pl.ds(s, rows), :] for s in starts], axis=0)
        for h in range(heads):
            cols = slice(h * HEAD_DIM, (h + 1) * HEAD_DIM)
            scores = lax.dot_general(
                q[:, cols], k[:, cols], (((1,), (1,)), ((), ())), preferred_element_type=F32
            )
            scores = scores / jnp.sqrt(F32(HEAD_DIM))
            scores = jnp.where(causal, scores, F32(-1e30))
            expo = jnp.exp(scores - jnp.max(scores, axis=-1, keepdims=True))
            probs = (expo / jnp.sum(expo, axis=-1, keepdims=True)).astype(BF16)
            none = jnp.zeros((seq, seq), BF16)
            pair = [probs, none] if h < half else [none, probs]
            out_ref[h, :, :] = jnp.concatenate(pair, axis=0)


def attention_probs(queries, keys, tensors):
    micro, seq, cols = queries.shape
    outs = [((cols // HEAD_DIM, 2 * seq, seq), BF16)] * micro
    flops = 4 * micro * seq * seq * cols
    kernel = functools.partial(probs_kernel, tensors)
    return run(kernel, outs, [queries, keys], [], flops, 4 * queries.size)


def ctx_matmul(weight_ref, terms, start_ref, out_ref):
    half = weight_ref.shape[0] // 2
    step = min(half, 384)
    dims = (((1,), (1,)), ((), ()))
    for at in range(0, half, step):
        sides = []
        for off in (0, half):
            rows = slice(at + off, at + off + step)
            total = None
            for cols, upper in terms:
                term = lax.dot_general(
                    weight_ref[rows, cols], upper, dims, preferred_element_type=F32
                )
                total = term if total is None else total + term
            sides.append(total)
        out = jnp.concatenate(sides, axis=1)
        if start_ref is not None:
            out = out + start_ref[at : at + step, :]
        out_ref[at : at + step, :] = out.astype(out_ref.dtype)


def first_kernel(m, *refs):
    blocks, (weight_ref, part_ref, near_ref, far_ref) = refs[:-4], refs[-4:]
    side = core_side()
    rows, width = blocks[0].shape[1:]
    near, far = part(side, width // 2), part(1 - side, width // 2)
    for flip, ref in enumerate(blocks):
        at = part(side ^ flip, rows)
        near_ref[at, :] = ref[m, :, near]
        far_ref[at, :] = ref[m, :, far]
    ctx_matmul(weight_ref, [(near, near_ref[...]), (far, far_ref[...])], None, part_ref)


def take_turn(taker, blocks, prev_ref, upper_ref):
    take = lax.axis_index("section") == taker
    rows = blocks[0].shape[0]
    for b, ref in enumerate(blocks):
        at = slice(b * rows, (b + 1) * rows)
        upper_ref[at, :] = jnp.where(take, ref[...], prev_ref[at, :])


def near_kernel(taker, *refs):
    blocks, (prev_ref, weight_ref, start_ref, upper_ref) = refs[:-4], refs[-4:]
    take_turn(taker, blocks, prev_ref, upper_ref)
    cols = part(core_side(), upper_ref.shape[1])
    ctx_matmul(weight_ref, [(cols, upper_ref[...])], None, start_ref)


def far_kernel(taker, *refs):
    blocks, (prev_ref, start_ref, weight_ref, part_ref, upper_ref) = refs[:-5], refs[-5:]
    take_turn(taker, blocks, prev_ref, upper_ref)
    cols = part(1 - core_side(), upper_ref.shape[1])
    ctx_matmul(weight_ref, [(cols, upper_ref[...])], start_ref, part_ref)


def first_ctx(m, blocks, weight, tokens, after):
    cols, width = weight.shape
    side = ((tokens, width // 2), BF16)
    outs = [((cols // 2, 2 * tokens), BF16), side, side]
    flops = 2 * tokens * cols * width
    kernel = functools.partial(first_kernel, m)
    return run(kernel, outs, [*blocks, weight], after, flops, 2 * weight.size)


def half_ctx(taker, blocks, prev, start, weight, after):
    cols, tokens = weight.shape[0], prev.shape[0]
    kernel = functools.partial(near_kernel if start is None else far_kernel, taker)
    starts = [] if start is None else [start]
    outs = [((cols // 2, 2 * tokens), F32 if start is None else BF16), (prev.shape, BF16)]
    operands = [*blocks, prev, *starts, weight]
    return run(kernel, outs, operands, after, 2 * cols * prev.size, weight.size)


def value_grads(terms, probs_ref, grad_ref):
    half = probs_ref.shape[0] // 2
    packed = terms[0][...].astype(F32)
    for ref in terms[1:]:
        packed = packed + ref[...].astype(F32)
    packed = packed.astype(BF16)
    for h in range(2 * half):
        row = (h % half) * HEAD_DIM
        grad = jnp.dot(
            packed[row : row + HEAD_DIM, :], probs_ref[h], preferred_element_type=F32
        )
        grad_ref[h * HEAD_DIM : (h + 1) * HEAD_DIM, :] = grad.astype(BF16)


def branch_rows(weight_ref, first, count, grads):
    step = min(count, 768)
    for at in range(0, count, step):
        rows = pl.ds(pl.multiple_of(first * count + at, 128), step)
        out = jnp.dot(weight_ref[rows, :], grads, preferred_element_type=F32)
        yield slice(at, at + step), out.T


def send_kernel(*refs):
    terms, (probs_ref, weight_ref, send_ref, grad_ref) = refs[:-4], refs[-4:]
    value_grads(terms, probs_ref, grad_ref)
    half = send_ref.shape[1]
    for at, out in branch_rows(weight_ref, 1 - core_side(), half, grad_ref[...]):
        send_ref[:, at] = out.astype(BF16)


def keep_kernel(grad_ref, weight_ref, keep_ref):
    half = keep_ref.shape[1]
    for at, out in branch_rows(weight_ref, core_side(), half, grad_ref[...]):
        keep_ref[:, at] = out


def send_branch(terms, probs, weight, after):
    width, cols = weight.shape
    tokens = probs.shape[2]
    outs = [((tokens, width // 2), BF16), ((cols, tokens), BF16)]
    flops = tokens * cols * width
    return run(send_kernel, outs, [*terms, probs, weight], after, flops, weight.size)


def keep_branch(grads, weight, after):
    width, cols = weight.shape
    tokens = grads.shape[1]
    outs = [((tokens, width // 2), F32)]
    flops = tokens * cols * width
    return run(keep_kernel, outs, [grads, weight], after, flops, weight.size)[0]


def last_kernel(rows, *refs):
    terms, (probs_ref, weight_ref, keep_ref, send_ref, grad_ref) = refs[:-5], refs[-5:]
    value_grads(terms, probs_ref, grad_ref)
    low = core_side() == 0
    for at, out in branch_rows(weight_ref, 0, keep_ref.shape[1], grad_ref[...]):
        for b in range(keep_ref.shape[0] // rows):
            one = out[2 * b * rows : (2 * b + 1) * rows]
            two = out[(2 * b + 1) * rows : (2 * b + 2) * rows]
            keep_ref[b * rows : (b + 1) * rows, at] = jnp.where(low, one, two)
            send_ref[b * rows : (b + 1) * rows, at] = jnp.where(low, two, one).astype(BF16)


def last_branch(terms, probs, weight, rows, after):
    width, cols = weight.shape
    tokens = probs.shape[2]
    half = (tokens // 2, width)
    outs = [(half, F32), (half, BF16), ((cols, tokens), BF16)]
    kernel = functools.partial(last_kernel, rows)
    flops = 2 * tokens * cols * width
    return run(kernel, outs, [*terms, probs, weight], after, flops, 2 * weight.size)


def pair_kernel(keep_ref, got_ref, mine_ref, *away_refs):
    total = keep_ref[...] + got_ref[...].astype(F32)
    rows = mine_ref.shape[0]
    mine_ref[...] = total[:rows]
    for b, ref in enumerate(away_refs, 1):
        ref[...] = total[b * rows : (b + 1) * rows].astype(BF16)


def pair_sum(keep, got, chips, after):
    total, width = keep.shape
    shape = (total // chips, width)
    outs = [(shape, F32)] + [(shape, BF16)] * (chips - 1)
    return run(pair_kernel, outs, [keep, got], after, keep.size, 6 * keep.size)


def whole_pair_kernel(keep_ref, got_ref, mine_ref, away_ref):
    mine = keep_ref[...] + got_ref[...].astype(F32)
    mine_ref[...] = mine
    away_ref[...] = mine.astype(BF16)


def whole_pair_sum(keep, got):
    outs = [(keep.shape, F32), (keep.shape, BF16)]
    return run(whole_pair_kernel, outs, [keep, got], [], keep.size, 6 * keep.size)


def fresh_kernel(*refs):
    mine_ref, heard, (upper_ref, out_ref) = refs[0], refs[1:-2], refs[-2:]
    chips = len(heard) + 1
    rows = mine_ref.shape[0] // chips
    for b in range(chips):
        at = slice(b * rows, (b + 1) * rows)
        total = mine_ref[at, :]
        for d, ref in enumerate(heard, 1):
            total = total + ref[(b ^ d) * rows : ((b ^ d) + 1) * rows, :].astype(F32)
        out_ref[at, :] = (total + upper_ref[at, :].astype(F32)).astype(BF16)


def fresh_rows(mine, heard, upper, after):
    operands = [mine, *heard, upper]
    outs = [(mine.shape, BF16)]
    return run(fresh_kernel, outs, operands, after, mine.size, 6 * mine.size)[0]


def result_kernel(micro, *refs):
    out_ref = refs[-1]
    rows, half = out_ref.shape[1], out_ref.shape[2] // 2
    each = (len(refs) - 1) // micro
    side = core_side()
    for m in range(micro):
        mine_ref, *heard, near_ref, far_ref = refs[m * each : (m + 1) * each]
        for upper_ref, cols in ((near_ref, part(side, half)), (far_ref, part(1 - side, half))):
            total = mine_ref[:, cols]
            for ref in heard:
                total = total + ref[:, cols].astype(F32)
            upper = upper_ref[part(side, rows), :].astype(F32)
            out_ref[m, :, cols] = (total + upper).astype(BF16)


def result_rows(mine, heard, uppers):
    micro, (rows, width) = len(mine), mine[0].shape
    operands = []
    for m in range(micro):
        operands += [mine[m], *heard[m], *uppers[m]]
    kernel = functools.partial(result_kernel, micro)
    size = micro * rows * width
    outs = [((micro, rows, width), BF16)]
    return run(kernel, outs, operands, [], size, 6 * size)[0]


def hold_kernel(src_ref, out_ref, sems):
    parts = sems.shape[0]
    rows = src_ref.shape[0] // parts
    copies = [
        pltpu.make_async_copy(
            src_ref.at[pl.ds(i * rows, rows), :], out_ref.at[pl.ds(i * rows, rows), :], sems.at[i]
        )
        for i in range(parts)
    ]
    for copy in copies:
        copy.start()
    for copy in copies:
        copy.wait()


def held(array):
    return pl.pallas_call(
        hold_kernel,
        out_shape=jax.ShapeDtypeStruct(array.shape, array.dtype),
        in_specs=[pl.BlockSpec(memory_space=pltpu.HBM)],
        out_specs=vmem(),
        scratch_shapes=[pltpu.SemaphoreType.DMA((8,))],
        compiler_params=params(4),
        cost_estimate=cost(array.size, 2 * array.size),
        name="held",
    )(pltpu.with_memory_space_constraint(array, pltpu.HBM))


def stream_product(lhs_of, rhs, out_ref, buf, sems):
    count = sems.shape[0]
    step = buf.shape[0] // count

    def copy(i):
        rows = pl.ds(pl.multiple_of(i * step, step), step)
        return pltpu.make_async_copy(buf.at[rows, :], out_ref.at[rows, :], sems.at[i])

    @pl.loop(0, count, unroll=2)
    def _(i):
        rows = pl.ds(pl.multiple_of(i * step, step), step)
        product = jnp.dot(lhs_of(rows).T, rhs, preferred_element_type=F32)
        buf[rows, :] = product.astype(BF16)
        copy(i).start()

    @pl.loop(0, count)
    def _(i):
        copy(i).wait()


def out_grad_kernel(tensors, ctx_ref, *refs):
    uppers, (out_ref, done_ref, buf, sems, _, rhs) = refs[:-6], refs[-6:]
    tokens, half = uppers[0].shape
    rows = tokens // tensors
    sides = (core_side(), 1 - core_side())
    for i, ref in enumerate(uppers):
        for b, block in enumerate(token_order(tensors)):
            at = pl.multiple_of((i // 2) * tokens + block * rows, rows)
            rhs[pl.ds(at, rows), part(sides[i % 2], half)] = ref[b * rows : (b + 1) * rows, :]
    stream_product(lambda at: ctx_ref[:, at], rhs[...], out_ref, buf, sems)
    done_ref[...] = jnp.zeros_like(done_ref)


def value_grad_kernel(micro, *refs):
    blocks, grads = refs[: -micro - 6], refs[-micro - 6 : -6]
    out_ref, done_ref, buf, sems, lhs, rhs = refs[-6:]
    tokens = grads[0].shape[1]
    rows = tokens // len(blocks)
    for m, ref in enumerate(grads):
        rhs[m * tokens : (m + 1) * tokens, :] = ref[...].T
        for flip, block in enumerate(blocks):
            at = pl.multiple_of(m * tokens + (core_side() ^ flip) * rows, rows)
            lhs[pl.ds(at, rows), :] = block[m]
    stream_product(lambda at: lhs[:, at], rhs[...], out_ref, buf, sems)
    done_ref[...] = jnp.zeros_like(done_ref)


def weight_grad(kernel, operands, shape, tokens, after):
    rows, cols = shape
    step = min(rows, 256)
    used = len(operands)

    def body(*refs):
        kernel(*refs[:used], *refs[used + len(after) :])

    return pl.pallas_call(
        body,
        out_shape=[jax.ShapeDtypeStruct(shape, BF16), jax.ShapeDtypeStruct((8, 128), F32)],
        in_specs=[vmem()] * (used + len(after)),
        out_specs=[pl.BlockSpec(memory_space=pltpu.HBM), vmem()],
        scratch_shapes=[
            pltpu.VMEM(shape, BF16),
            pltpu.SemaphoreType.DMA((rows // step,)),
            pltpu.VMEM((tokens, rows), BF16),
            pltpu.VMEM((tokens, cols), BF16),
        ],
        compiler_params=params(20),
        cost_estimate=cost(2 * tokens * rows * cols, 2 * rows * cols),
    )(*operands, *after)


def per_device(cotangent, inputs, queries, keys, context, value_weight, out_weight):
    sections = lax.axis_size("section")
    tensors = lax.axis_size("tensor")
    replicas = lax.axis_size("dp")
    micro, rows, width = cotangent.shape
    seq, cols = queries.shape[2:]
    value_proj = value_weight[0]
    turns = range(0, tensors, 2)

    def gathered(block):
        near = [block] + [across(block, "tensor", f) for f in turns[1:]]
        far = [across(n, "tensor", 1) for n in near]
        return [b for both in zip(near, far) for b in both]

    def each():
        return [None] * micro

    first = gathered(cotangent)
    probs = attention_probs(queries[0], keys[0], tensors)
    out_proj = held(out_weight[0])
    parts, nears, fars, grads = each(), each(), each(), each()
    last = list(probs[:1])
    for m in range(micro):
        parts[m], nears[m], fars[m] = first_ctx(m, first, out_proj, seq, last)
        last = [parts[m]]
    in_blocks = gathered(inputs[0])
    for stage in range(sections):
        ending = stage == sections - 1
        mine, heard = each(), each()
        if ending:
            uppers = list(zip(nears, fars))
            out_w, done = weight_grad(
                functools.partial(out_grad_kernel, tensors),
                [
                    context[0].reshape(micro * seq, cols),
                    *(side for both in uppers for side in both),
                ],
                (cols, width),
                micro * seq,
                last,
            )
            last = [done]
        for m in range(micro):
            terms = [parts[m]] + [across(parts[m], "dp", d) for d in range(1, replicas)]
            if ending:
                keep, send, grads[m] = last_branch(terms, probs[m], value_proj, rows, last)
                got = across(send, "tensor", 1)
            else:
                send, grads[m] = send_branch(terms, probs[m], value_proj, last)
                got = across(send, "tensor", 1)
                keep = keep_branch(grads[m], value_proj, [send])
            if ending:
                mine[m], *away = pair_sum(keep, got, tensors // 2, [])
                last = [send]
            else:
                mine[m], away = whole_pair_sum(keep, got)
                away = [away] * (tensors // 2 - 1)
                last = [mine[m]]
            heard[m] = [across(a, "tensor", f) for a, f in zip(away, turns[1:])]
        if ending:
            break
        fresh = each()
        last = last + (in_blocks[2::2] if stage == 0 else in_blocks[1::2] if stage == 1 else [])
        for m in range(micro):
            fresh[m] = fresh_rows(mine[m], heard[m], nears[m], last)
            last = [fresh[m]]
        for m in range(micro):
            near = [below(fresh[m], sections - 1 - stage)]
            far = [across(n, "tensor", 1) for n in near]
            taker = sections - 2 - stage
            start, nears[m] = half_ctx(taker, near, nears[m], None, out_proj, last)
            parts[m], fars[m] = half_ctx(taker, far, fars[m], start, out_proj, [])
            last = [parts[m]]
    result = result_rows(mine, heard, uppers)
    value_w, _ = weight_grad(
        functools.partial(value_grad_kernel, micro),
        [*in_blocks, *grads],
        (width, cols),
        micro * seq,
        mine,
    )
    return (result[None], value_w[None], out_w[None])


def solution(mesh):
    placed = (
        P(None, "tensor", "dp"),
        P("section", None, "tensor", "dp"),
        P("section", None, None, "tensor"),
        P("section", None, None, "tensor"),
        P("section", None, None, "tensor"),
        P("section", "dp", "tensor"),
        P("section", "tensor", "dp"),
    )
    return jax.shard_map(
        per_device,
        mesh=mesh,
        in_specs=placed,
        out_specs=(
            P("section", None, "tensor", "dp"),
            P("section", "dp", "tensor"),
            P("section", "tensor", "dp"),
        ),
        check_vma=False,
    )
```
